32 devices in a mesh: dp: 4 (over z), mp: 8 (over y, x, core).
Axes of the slice: x: 2, y: 2, z: 4, core: 2. Of those that a mesh axis runs over, the one named last changes fastest.
Arguments:
- tokens: bfloat16 [21376, 1152], P(('dp', 'mp')), may hold values from -6 to 6
- skip_tokens: bfloat16 [21376, 1152], P(('dp', 'mp')), may hold values from -6 to 6
- caption_lengths: int32 [64], P('dp'), may hold values from 1 to 77
- output_cotangent: bfloat16 [21376, 1152], P(('dp', 'mp')), may hold values from -6 to 6
- skip_weight: bfloat16 [2304, 1152], P(('dp', 'mp')), may hold values from -0.125 to 0.125
- norm_gains: bfloat16 [2, 1152], P(None, ('dp', 'mp')), may hold values from 0.099609375 to 1.8984375
- bias_rows: bfloat16 [5, 1152], P(None, ('dp', 'mp')), may hold values from -3 to 3
- input_weight: bfloat16 [1152, 3, 1152], P('dp', None, 'mp'), may hold values from -0.25 to 0.25
- output_weight: bfloat16 [1152, 1152], P('mp', 'dp'), may hold values from -0.5 to 0.5
- up_weight: bfloat16 [1152, 4608], P('dp', 'mp'), may hold values from -0.1875 to 0.1875
- up_bias: bfloat16 [4608], P(('mp', 'dp')), may hold values from -3 to 3
- down_weight: bfloat16 [4608, 1152], P('mp', 'dp'), may hold values from -0.125 to 0.125
Outputs:
- output: bfloat16 [21376, 1152], P(('dp', 'mp'))
- grad_tokens: bfloat16 [21376, 1152], P(('dp', 'mp'))
- grad_skip_tokens: bfloat16 [21376, 1152], P(('dp', 'mp'))
- grad_skip_weight: float32 [2304, 1152], P(('dp', 'mp'))
- grad_norm_gains: float32 [2, 1152], P(None, ('dp', 'mp'))
- grad_bias_rows: float32 [5, 1152], P(None, ('dp', 'mp'))
- grad_input_weight: float32 [1152, 3, 1152], P('dp', None, 'mp')
- grad_output_weight: float32 [1152, 1152], P('mp', 'dp')
- grad_up_weight: float32 [1152, 4608], P('dp', 'mp')
- grad_up_bias: float32 [4608], P(('mp', 'dp'))
- grad_down_weight: float32 [4608, 1152], P('mp', 'dp')
The draws below stay inside these ranges and needn't reach their ends.
All inputs are finite; a program needn't handle non-finite values.
Results may differ from the reference program's by a relative error of at most 0.023.
Values may be sent and summed in bfloat16 or wider, within the bound.
A program may use at most 256 MiB of HBM per device.

```python
import jax
import jax.numpy as jnp
from jax import lax

D = 1152
H = 16
HD = 72
F = 4608
CAP = 77
SEQ = 334
ITEMS = 64
TOKENS = 21376


def with_ends(entries, own_key, least, largest):
    place = [jax.random.randint(jax.random.fold_in(own_key, axis), (), 0, length) for axis, length in enumerate(entries.shape)]
    longest = entries.shape.index(max(entries.shape))
    next_to = place[:longest] + [(place[longest] + 1) % entries.shape[longest]] + place[longest + 1:]
    return entries.at[tuple(place)].set(least).at[tuple(next_to)].set(largest)


def steps_of(own_key, extent, split, least, largest):
    factor_of, own = 1.0, jax.random.fold_in(own_key, 6)
    for position, shards_of in split:
        draws = jnp.exp(jax.random.uniform(jax.random.fold_in(own, position), (shards_of,), jnp.float32, least / len(split), largest / len(split)))
        factor_of = factor_of * jnp.repeat(draws, extent[position] // shards_of).reshape([-1 if axis == position else 1 for axis in range(len(extent))])
    return factor_of


def gaussian(key, dims, scale, reach, split=(), kind=jnp.bfloat16):
    entries = jax.random.normal(key, dims, jnp.float32) * scale
    if len(split) > 0:
        entries = steps_of(key, dims, split, -0.22, 0.18) * entries
    return jnp.clip(entries, min=-reach, max=reach).astype(kind)


def setup_inputs(seed: int = 0) -> dict:
    keys = jax.random.split(jax.random.key(seed), 13)
    tokens = gaussian(keys[0], (TOKENS, D), 1.0, 6.0, ((0, 32),))
    skip_tokens = gaussian(keys[1], (TOKENS, D), 1.0, 6.0, ((0, 32),))
    caption_lengths = with_ends(jax.random.randint(keys[2], (ITEMS,), 1, CAP + 1), jax.random.fold_in(keys[2], 1), 1, CAP).astype(jnp.int32)
    output_cotangent = gaussian(keys[3], (TOKENS, D), 1.0, 6.0, ((0, 32),))
    skip_weight = gaussian(keys[4], (2 * D, D), (2 * D) ** -0.5, 0.125, ((0, 32),))
    norm_gains = jnp.clip(1.0 + 0.18 * jax.random.normal(keys[5], (2, D), jnp.float32), 0.099609375, 1.8984375).astype(jnp.bfloat16)
    bias_rows = gaussian(keys[6], (5, D), 0.5, 3.0, ((1, 32),))
    input_weight = gaussian(keys[7], (D, 3, D), (D // 2) ** -0.5, 0.25, ((0, 4), (2, 8)))
    output_weight = gaussian(keys[8], (D, D), (D // 8) ** -0.5, 0.5, ((0, 8), (1, 4)))
    up_weight = gaussian(keys[9], (D, F), D ** -0.5, 0.1875, ((0, 4), (1, 8)))
    up_bias = gaussian(keys[10], (F,), 0.5, 3.0, ((0, 32),))
    down_weight = gaussian(keys[11], (F, D), (F // 2) ** -0.5, 0.125, ((0, 8), (1, 4)))
    return dict(tokens=tokens, skip_tokens=skip_tokens, caption_lengths=caption_lengths, output_cotangent=output_cotangent, skip_weight=skip_weight, norm_gains=norm_gains, bias_rows=bias_rows, input_weight=input_weight, output_weight=output_weight, up_weight=up_weight, up_bias=up_bias, down_weight=down_weight)


@jax.custom_vjp
def low(v):
    return lax.optimization_barrier(v.astype(jnp.bfloat16)).astype(jnp.float32)

@jax.custom_vjp
def low_back(v):
    return v

def low_keep(v):
    return (low(v), None)

def low_pass(kept, grad):
    return (grad,)

def back_keep(v):
    return (v, None)

def back_low(kept, grad):
    return (low(grad),)
low.defvjp(low_keep, low_pass)
low_back.defvjp(back_keep, back_low)
exact_mode = lax.Precision.HIGHEST
norm_eps = 1e-05
masked_score = -1e+30

def layer_norm(values, weight, offset):
    average = lax.optimization_barrier(jnp.mean(values, -1, keepdims=True))
    centred = values - average
    spread = lax.optimization_barrier(jnp.mean(centred * centred, -1, keepdims=True))
    return centred * lax.rsqrt(spread + norm_eps) * weight + offset

def block_forward(params, token_rows, skip_rows, key_valid):
    skip_weight, norm_gains, bias_rows, input_weight, output_weight, up_weight, up_bias, down_weight = params
    joined = jnp.concatenate([token_rows, skip_rows], axis=1)
    hidden = low_back(jnp.dot(joined, skip_weight, precision=exact_mode) + bias_rows[0])
    normed = low(layer_norm(hidden, norm_gains[0], bias_rows[1]))
    triples = low(low_back(jnp.einsum('td,dcn->tcn', normed, input_weight, precision=exact_mode)))
    row_total = normed.shape[0]
    shaped = triples.reshape(row_total // SEQ, SEQ, 3, H, HD)
    scores = jnp.einsum('bqhd,bkhd->bhqk', shaped[:, :, 0], shaped[:, :, 1], precision=exact_mode)
    scores = low_back(scores * HD ** (-0.5))
    scores = jnp.where(key_valid[:, None, None, :], scores, masked_score)
    prob_rows = low(jax.nn.softmax(scores, axis=-1))
    mixed_rows = jnp.einsum('bhqk,bkhd->bqhd', prob_rows, shaped[:, :, 2], precision=exact_mode)
    mixed_rows = low(low_back(mixed_rows)).reshape(row_total, H * HD)
    attention = low_back(jnp.dot(mixed_rows, output_weight, precision=exact_mode) + bias_rows[2])
    middle = hidden + attention
    normed_two = low(layer_norm(middle, norm_gains[1], bias_rows[3]))
    before = low_back(jnp.dot(normed_two, up_weight, precision=exact_mode) + up_bias)
    active = low(jax.nn.gelu(before, approximate=False))
    branch = low_back(jnp.dot(active, down_weight, precision=exact_mode) + bias_rows[4])
    return middle + branch

def reference(tokens, skip_tokens, caption_lengths, output_cotangent, skip_weight, norm_gains, bias_rows, input_weight, output_weight, up_weight, up_bias, down_weight):
    params = tuple((weight.astype(jnp.float32) for weight in (skip_weight, norm_gains, bias_rows, input_weight, output_weight, up_weight, up_bias, down_weight)))
    item_total = caption_lengths.shape[0]
    per_group = max((option for option in range(1, item_total + 1) if item_total % option == 0 and option * SEQ <= 4096))
    group_total = item_total // per_group
    feature_total = tokens.shape[1]

    def regroup(values):
        return values.astype(jnp.float32).reshape(group_total, per_group * SEQ, feature_total)
    positions = jnp.arange(SEQ, dtype=jnp.int32)

    def scan_step(totals, packed):
        token_rows, skip_rows, length_rows, grad_rows = packed
        key_valid = (positions[None, :] < 1) | (positions[None, :] > CAP) | (positions[None, :] - 1 < length_rows[:, None])

        def forward(weights, token_part, skip_part):
            return block_forward(weights, token_part, skip_part, key_valid)
        result, pullback = jax.vjp(forward, params, token_rows, skip_rows)
        grad_params, grad_token_rows, grad_skip_rows = pullback(grad_rows)
        totals = jax.tree.map(lambda earlier, latest: earlier + latest, totals, grad_params)
        return (totals, (result.astype(jnp.bfloat16), grad_token_rows.astype(jnp.bfloat16), grad_skip_rows.astype(jnp.bfloat16)))
    zero_grads = jax.tree.map(jnp.zeros_like, params)
    totals, stacked = lax.scan(scan_step, zero_grads, (regroup(tokens), regroup(skip_tokens), caption_lengths.reshape(group_total, per_group), regroup(output_cotangent)))

    def flatten_rows(values):
        return values.reshape(item_total * SEQ, feature_total)
    return (flatten_rows(stacked[0]), flatten_rows(stacked[1]), flatten_rows(stacked[2]), totals[0], totals[1], totals[2], totals[3], totals[4], totals[5], totals[6], totals[7])
```

```python
import functools

import jax
import jax.numpy as jnp
from jax import lax
from jax.experimental import pallas as pl
from jax.experimental.pallas import tpu as pltpu
from jax.sharding import PartitionSpec as P


HD = 72
CAP = 77
SEQ = 334
EPS = 1e-05
MASKED = -1e30
VMEM_BYTES = 60 * 1024 * 1024


bf16, f32 = jnp.bfloat16, jnp.float32


def dot_nn(a, b):
    return lax.dot_general(a, b, (((1,), (0,)), ((), ())), preferred_element_type=f32)


def dot_nt(a, b):
    return lax.dot_general(a, b, (((1,), (1,)), ((), ())), preferred_element_type=f32)


def dot_tn(a, b):
    return lax.dot_general(a, b, (((0,), (0,)), ((), ())), preferred_element_type=f32)


def tiles_of(extent, tile):
    return extent // tile, extent % tile


def gelu_parts(v):
    a = jnp.abs(v) * 0.7071067811865476
    t = 1.0 / (1.0 + 0.3275911 * a)
    e = jnp.exp(-a * a)
    poly = t * (
        0.254829592
        + t * (-0.284496736 + t * (1.421413741 + t * (-1.453152027 + t * 1.061405429)))
    )
    half = 0.5 * poly * e
    return jnp.where(v < 0, half, 1.0 - half), e * 0.3989422804014327


def ffn_kernel(first, n2, dy, b0, b1, ub, br_in, *rest):
    if first:
        gn_in = None
        br, gn, g0, g1, gub, wu, wd, gu, gd = rest
    else:
        gn_in, br, gn, g0, g1, gub, wu, wd, gu, gd = rest
    h = b0.shape[0] // 2
    wu[:h], wu[h:] = b0[:h], b1[:h]
    wd[:h], wd[h:] = b0[h:], b1[h:]
    br[...] = br_in[...]
    gn[...] = jnp.zeros(gn.shape, f32) if first else gn_in[...]

    def tile(start, size):
        w_up, w_down = wu[pl.ds(start, size), :], wd[pl.ds(start, size), :]
        before = dot_nt(n2[...], w_up) + ub[:, pl.ds(start, size)]
        grad_active = dot_nt(dy[...], w_down)
        cdf, pdf = gelu_parts(before)
        active = (before * cdf).astype(bf16)
        grad_f32 = grad_active * (cdf + before * pdf)
        grad_before = grad_f32.astype(bf16)
        br[...] += dot_nn(active, w_down)
        gn[...] += dot_nn(grad_before, w_up)
        gd[pl.ds(start, size), :] = dot_tn(active, dy[...]).astype(bf16)
        gu[pl.ds(start, size), :] = dot_tn(grad_before, n2[...]).astype(bf16)
        gub[:, pl.ds(start, size)] = jnp.sum(grad_before.astype(f32), 0, keepdims=True)

    size = 256
    count, left = tiles_of(2 * h, size)

    def step(i, carry):
        tile(pl.multiple_of(i * size, size), size)
        return carry

    lax.fori_loop(0, count, step, 0)
    if left:
        tile(count * size, left)
    g0[:h], g1[:h] = gu[:h], gu[h:]
    g0[h:], g1[h:] = gd[:h], gd[h:]


def ffn_pair(n2, dy, b0, b1, ub, br, gn):
    m, d = n2.shape
    h = b0.shape[0] // 2
    block = jax.ShapeDtypeStruct((2 * h, d), bf16)
    acc = jax.ShapeDtypeStruct((m, d), f32)
    vmem = pl.BlockSpec(memory_space=pltpu.VMEM)
    first = gn is None
    args = (n2, dy, b0, b1, ub, br) + (() if first else (gn,))
    return pl.pallas_call(
        functools.partial(ffn_kernel, first),
        out_shape=(acc, acc, block, block, jax.ShapeDtypeStruct((1, 2 * h), f32)),
        in_specs=[vmem] * len(args),
        out_specs=(vmem,) * 5,
        scratch_shapes=[pltpu.VMEM((2 * h, d), bf16)] * 4,
        compiler_params=pltpu.CompilerParams(vmem_limit_bytes=VMEM_BYTES),
        cost_estimate=pl.CostEstimate(
            flops=24 * m * d * h, bytes_accessed=20 * m * d + 16 * h * d, transcendentals=0
        ),
        name="ffn_pair",
    )(*args)


def windows(items):
    out = []
    for i in range(items):
        lo, hi = i * SEQ, (i + 1) * SEQ
        out.append((lo // 16 * 16, -(-hi // 16) * 16, lo, hi))
    return out


def key_mask(length, start, stop, lo, hi):
    row = lax.broadcasted_iota(jnp.int32, (1, stop - start), 1) + start
    pos = row - lo
    own = (row >= lo) & (row < hi)
    return own & ((pos < 1) | (pos > CAP) | (pos - 1 < length))


def put(ref, index, start, lo, value):
    stop = start + value.shape[0]
    if start == lo:
        ref[index, start:stop, :] = value
        return
    edge = start + 16
    row = lax.broadcasted_iota(jnp.int32, (16, 1), 0) + start
    kept = ref[index, start:edge, :]
    ref[index, start:edge, :] = jnp.where(row >= lo, value[:16], kept)
    ref[index, edge:stop, :] = value[16:]


def offsets(hw):
    out = []
    for b in range(2):
        for hh in range(hw // HD):
            out.append(
                (
                    b * 2 * hw + hh * HD,
                    b * 2 * hw + hw + hh * HD,
                    4 * hw + b * hw + hh * HD,
                    b * hw + hh * HD,
                )
            )
    return out


def softmax_parts(q, k, valid):
    s = jnp.where(valid, dot_nt(q, k), MASKED)
    top = jnp.max(s, -1, keepdims=True)
    e = jnp.exp((s - top) * HD ** (-0.5))
    return e * (1.0 / jnp.sum(e, -1, keepdims=True))


def load_pair(b0, b1, wq, wo):
    hw = b0.shape[0] // 4
    wq[: 2 * hw], wq[2 * hw : 4 * hw] = b0[: 2 * hw], b1[: 2 * hw]
    wq[4 * hw : 5 * hw], wq[5 * hw :] = b0[2 * hw : 3 * hw], b1[2 * hw : 3 * hw]
    wo[:hw], wo[hw:] = b0[3 * hw :], b1[3 * hw :]


def attend_kernel(items, lens, normed, b0, b1, acc_in, acc, qkv, mixed, wq, wo, slab, oslab):
    hw = b0.shape[0] // 4
    heads = 2 * hw // HD
    load_pair(b0, b1, wq, wo)
    qkv[...] = dot_nt(normed[...], wq[...]).astype(bf16)
    places = offsets(hw)
    for n, place in enumerate(places):
        for part in range(3):
            slab[part * heads + n] = qkv[:, place[part] : place[part] + HD]

    def step(n, carry):
        for i, (start, stop, lo, hi) in enumerate(windows(items)):
            valid = key_mask(lens[i], start, stop, lo, hi)
            q = slab[n, start:stop, :]
            k = slab[heads + n, start:stop, :]
            v = slab[2 * heads + n, start:stop, :]
            prob = softmax_parts(q, k, valid).astype(bf16)
            put(oslab, n, start, lo, dot_nn(prob, v).astype(bf16))
        return carry

    lax.fori_loop(0, heads, step, 0)
    for n, place in enumerate(places):
        mixed[:, place[3] : place[3] + HD] = oslab[n]
    acc[...] = acc_in[...] + dot_nn(mixed[...], wo[...])


def attend_pair(lens, normed, b0, b1, acc):
    m, d = normed.shape
    hw = b0.shape[0] // 4
    heads = 2 * hw // HD
    items = m // SEQ
    vmem = pl.BlockSpec(memory_space=pltpu.VMEM)
    return pl.pallas_call(
        functools.partial(attend_kernel, items),
        out_shape=(
            jax.ShapeDtypeStruct((m, d), f32),
            jax.ShapeDtypeStruct((m, 6 * hw), bf16),
            jax.ShapeDtypeStruct((m, 2 * hw), bf16),
        ),
        in_specs=[pl.BlockSpec(memory_space=pltpu.SMEM)] + [vmem] * 4,
        out_specs=(vmem,) * 3,
        scratch_shapes=[
            pltpu.VMEM((6 * hw, d), bf16),
            pltpu.VMEM((2 * hw, d), bf16),
            pltpu.VMEM((3 * heads, m, HD), bf16),
            pltpu.VMEM((heads, m, HD), bf16),
        ],
        compiler_params=pltpu.CompilerParams(vmem_limit_bytes=VMEM_BYTES),
        cost_estimate=pl.CostEstimate(
            flops=16 * m * d * hw + 4 * heads * m * SEQ * 256,
            bytes_accessed=10 * m * d + 16 * hw * d + 16 * m * hw,
            transcendentals=0,
        ),
        name="attend_pair",
    )(lens, normed, b0, b1, acc)


def attend_back_kernel(
    items, first, lens, normed, ga, b0, b1, qkv, mixed, *rest
):
    if first:
        gn_in = None
        gn, g0, g1, wq, wo, slab, gslab, gt = rest
    else:
        gn_in, gn, g0, g1, wq, wo, slab, gslab, gt = rest
    hw = b0.shape[0] // 4
    heads = 2 * hw // HD
    load_pair(b0, b1, wq, wo)
    grad_mixed = dot_nt(ga[...], wo[...]).astype(bf16)
    places = offsets(hw)
    for n, place in enumerate(places):
        for part in range(3):
            slab[part * heads + n] = qkv[:, place[part] : place[part] + HD]
        slab[3 * heads + n] = grad_mixed[:, place[3] : place[3] + HD]
    scale = HD ** (-0.5)

    def step(n, carry):
        for i, (start, stop, lo, hi) in enumerate(windows(items)):
            valid = key_mask(lens[i], start, stop, lo, hi)
            row = lax.broadcasted_iota(jnp.int32, (stop - start, 1), 0) + start
            q = slab[n, start:stop, :]
            k = slab[heads + n, start:stop, :]
            v = slab[2 * heads + n, start:stop, :]
            go = slab[3 * heads + n, start:stop, :].astype(f32)
            go = jnp.where((row >= lo) & (row < hi), go, 0.0).astype(bf16)
            prob = softmax_parts(q, k, valid)
            grad_prob = dot_nt(go, v)
            inner = jnp.sum(prob * grad_prob, -1, keepdims=True)
            grad_score = (prob * (grad_prob - inner)).astype(bf16)
            put(gslab, n, start, lo, (dot_nn(grad_score, k) * scale).astype(bf16))
            put(gslab, heads + n, start, lo, (dot_tn(grad_score, q) * scale).astype(bf16))
            put(gslab, 2 * heads + n, start, lo, dot_tn(prob.astype(bf16), go).astype(bf16))
        return carry

    lax.fori_loop(0, heads, step, 0)
    for n, place in enumerate(places):
        for part in range(3):
            gt[:, place[part] : place[part] + HD] = gslab[part * heads + n]
    total = dot_nn(gt[...], wq[...])
    gn[...] = total if first else gn_in[...] + total
    g0[: 2 * hw] = dot_tn(gt[:, : 2 * hw], normed[...]).astype(bf16)
    g1[: 2 * hw] = dot_tn(gt[:, 2 * hw : 4 * hw], normed[...]).astype(bf16)
    grad_v = dot_tn(gt[:, 4 * hw :], normed[...]).astype(bf16)
    grad_o = dot_tn(mixed[...], ga[...]).astype(bf16)
    g0[2 * hw : 3 * hw], g0[3 * hw :] = grad_v[:hw], grad_o[:hw]
    g1[2 * hw : 3 * hw], g1[3 * hw :] = grad_v[hw:], grad_o[hw:]


def attend_back_pair(lens, normed, ga, b0, b1, qkv, mixed, gn):
    m, d = normed.shape
    hw = b0.shape[0] // 4
    heads = 2 * hw // HD
    items = m // SEQ
    vmem = pl.BlockSpec(memory_space=pltpu.VMEM)
    block = jax.ShapeDtypeStruct((4 * hw, d), bf16)
    first = gn is None
    args = (lens, normed, ga, b0, b1, qkv, mixed) + (() if first else (gn,))
    return pl.pallas_call(
        functools.partial(attend_back_kernel, items, first),
        out_shape=(jax.ShapeDtypeStruct((m, d), f32), block, block),
        in_specs=[pl.BlockSpec(memory_space=pltpu.SMEM)] + [vmem] * (len(args) - 1),
        out_specs=(vmem,) * 3,
        scratch_shapes=[
            pltpu.VMEM((6 * hw, d), bf16),
            pltpu.VMEM((2 * hw, d), bf16),
            pltpu.VMEM((4 * heads, m, HD), bf16),
            pltpu.VMEM((3 * heads, m, HD), bf16),
            pltpu.VMEM((m, 6 * hw), bf16),
        ],
        compiler_params=pltpu.CompilerParams(vmem_limit_bytes=VMEM_BYTES),
        cost_estimate=pl.CostEstimate(
            flops=32 * m * d * hw + 10 * heads * m * SEQ * 256,
            bytes_accessed=12 * m * d + 24 * hw * d + 16 * m * hw,
            transcendentals=0,
        ),
        name="attend_back_pair",
    )(*args)


def norm_parts(values):
    centred = values - jnp.mean(values, -1, keepdims=True)
    inv = lax.rsqrt(jnp.mean(centred * centred, -1, keepdims=True) + EPS)
    return centred * inv, inv


def norm_back(unit, inv, gain, grad):
    e = grad * gain
    return inv * (e - jnp.mean(e, -1, keepdims=True) - unit * jnp.mean(e * unit, -1, keepdims=True))


def swap(value, bit, size):
    return lax.ppermute(value, "mp", [(i, i ^ bit) for i in range(size)])


def orders(size):
    bits = [1 << n for n in range(1, size.bit_length() - 1)]
    return bits + [1], bits[::-1] + [1]


def gather_blocks(block, order, size):
    blocks = {0: block}
    for bit in order:
        for j in list(blocks):
            blocks[j | bit] = swap(blocks[j], bit, size)
    return blocks


def add(*values):
    return functools.reduce(jnp.add, [v.astype(f32) for v in values])


def scatter_blocks(blocks, order, size):
    blocks = dict(blocks)
    for bit in reversed(order):
        for j in sorted(blocks, reverse=True):
            if j & bit:
                got = swap(blocks.pop(j), bit, size)
                blocks[j ^ bit] = add(blocks[j ^ bit], got).astype(bf16)
    return blocks[0]


def core_sums(blocks, size):
    out = {}
    for j in sorted(blocks, reverse=True):
        if j & 1:
            got = swap(blocks[j], 1, size)
            out[j ^ 1] = add(blocks[j ^ 1], got).astype(bf16)
    return out


def line_gather(value):
    n, z = lax.axis_size("dp"), lax.axis_index("dp")
    bit = 1
    while bit < n:
        other = lax.ppermute(value, "dp", [(i, i ^ bit) for i in range(n)])
        high = (z & bit) != 0
        value = jnp.concatenate(
            [jnp.where(high, other, value), jnp.where(high, value, other)], 0
        )
        bit *= 2
    return value


def line_scatter(blocks):
    n, z = lax.axis_size("dp"), lax.axis_index("dp")
    bit = n // 2
    while bit:
        place = jnp.where((z & bit) != 0, bit, 0)
        kept = lax.dynamic_slice_in_dim(blocks, place, bit, 0)
        sent = lax.dynamic_slice_in_dim(blocks, bit - place, bit, 0)
        got = lax.ppermute(sent, "dp", [(i, i ^ bit) for i in range(n)])
        blocks = add(kept, got)
        bit //= 2
        if bit:
            blocks = blocks.astype(bf16)
    return blocks[0]


def shards(
    tokens,
    skip_tokens,
    caption_lengths,
    output_cotangent,
    skip_weight,
    norm_gains,
    bias_rows,
    input_weight,
    output_weight,
    up_weight,
    up_bias,
    down_weight,
):
    dp, mp = lax.axis_size("dp"), lax.axis_size("mp")
    my = lax.axis_index("mp")
    rows, d = tokens.shape
    items = rows // SEQ
    m = -(-rows // 16) * 16
    hw = input_weight.shape[2]
    part = skip_weight.shape[0]
    cols = norm_gains.shape[1]
    hidden_part = up_bias.shape[0]
    h = up_weight.shape[1]
    order_a, order_b = orders(mp)

    vector = jnp.concatenate([norm_gains.reshape(-1), bias_rows.reshape(-1), up_bias])
    vector = jnp.pad(vector, (0, d - vector.shape[0])).reshape(1, d)
    extra = jnp.pad(vector, ((0, 7), (0, 0)))
    packed = jnp.concatenate([skip_weight, extra], 0)
    span = packed.shape[0]
    skip_block = line_gather(packed)
    attn_part = jnp.concatenate([input_weight.reshape(-1, 3 * hw), output_weight.T], 1)
    attn_block = line_gather(attn_part).T
    ffn_part = jnp.concatenate([up_weight, down_weight.T], 1)
    ffn_block = line_gather(ffn_part).T

    skip = gather_blocks(skip_block, order_a[:-1], mp)
    own_core = jnp.stack([skip[j] for j in sorted(skip)])
    other_core = swap(own_core, 1, mp)
    attn = gather_blocks(attn_block, order_a, mp)
    ffn = gather_blocks(ffn_block, order_b, mp)

    whole_skip = jnp.zeros((dp, mp, part, d), bf16)
    whole_vec = jnp.zeros((dp, mp, 7, cols), bf16)
    shifts_up = {}
    for j in range(mp):
        piece = (other_core if j & 1 else own_core)[j // 2].reshape(dp, span, d)
        whole_skip = lax.dynamic_update_slice(
            whole_skip, piece[:, None, :part], (0, my ^ j, 0, 0)
        )
        line = piece[:, part]
        whole_vec = lax.dynamic_update_slice(
            whole_vec, line[:, : 7 * cols].reshape(dp, 1, 7, cols), (0, my ^ j, 0, 0)
        )
        shifts_up[j] = line[:, 7 * cols : 7 * cols + hidden_part].reshape(1, -1).astype(f32)
    whole_skip = whole_skip.reshape(2 * d, d)
    vectors = whole_vec.transpose(2, 0, 1, 3).reshape(7, d).astype(f32)
    gains, shift = vectors[:2], vectors[2:]

    pad = ((0, m - rows), (0, 0))
    tok, skp, dy = jnp.pad(tokens, pad), jnp.pad(skip_tokens, pad), jnp.pad(output_cotangent, pad)
    lens = lax.dynamic_slice(caption_lengths, (my * items,), (items,))
    joined = jnp.concatenate([tok, skp], 1)
    hidden = jnp.dot(joined, whole_skip, preferred_element_type=f32) + shift[0]
    unit_one, inv_one = norm_parts(hidden)
    normed = (unit_one * gains[0] + shift[1]).astype(bf16)

    middle = hidden + shift[2]
    kept = {}
    pairs = [0, *range(2, mp, 2)]
    for j in pairs:
        middle, qkv, mixed = attend_pair(lens, normed, attn[j], attn[j + 1], middle)
        kept[j] = (qkv, mixed)
    unit_two, inv_two = norm_parts(middle)
    normed_two = (unit_two * gains[1] + shift[3]).astype(bf16)

    result, grad_two = middle + shift[4], None
    grad_ffn, grad_up_bias = {}, {}
    for j in pairs:
        ub = jnp.concatenate([shifts_up[j], shifts_up[j + 1]], 1)
        result, grad_two, grad_ffn[j], grad_ffn[j + 1], gub = ffn_pair(
            normed_two, dy, ffn[j], ffn[j + 1], ub, result, grad_two
        )
        gub = gub.reshape(2, dp, hidden_part)
        grad_up_bias[j], grad_up_bias[j + 1] = gub[0], gub[1]
    output = result[:rows].astype(bf16)
    chip_ffn = core_sums(grad_ffn, mp)
    own_up = scatter_blocks({j: v[:h] for j, v in chip_ffn.items()}, order_a[:-1], mp)
    own_down = scatter_blocks({j: v[h:] for j, v in chip_ffn.items()}, order_b[:-1], mp)
    own_ffn = jnp.concatenate([own_up, own_down], 0)
    ffn_grads = line_scatter(own_ffn.T.reshape(dp, -1, 2 * h))
    up_grads, down_grads = ffn_grads[:, :h], ffn_grads[:, h:].T

    dy32 = dy.astype(f32)
    grad_middle = dy32 + norm_back(unit_two, inv_two, gains[1], grad_two)
    grad_attention = grad_middle.astype(bf16)

    grad_one = None
    grad_attn = {}
    for j in reversed(pairs):
        grad_one, grad_attn[j], grad_attn[j + 1] = attend_back_pair(
            lens, normed, grad_attention, attn[j], attn[j + 1], *kept[j], grad_one
        )
    own_attn = scatter_blocks(grad_attn, order_a, mp)
    attn_grads = line_scatter(own_attn.T.reshape(dp, -1, 4 * hw))
    in_grads = attn_grads[:, : 3 * hw].reshape(-1, 3, hw)
    out_grads = attn_grads[:, 3 * hw :].T

    grad_hidden = (grad_middle + norm_back(unit_one, inv_one, gains[0], grad_one)).astype(bf16)
    grad_skip = lax.dot_general(
        joined, grad_hidden, (((0,), (0,)), ((), ())), preferred_element_type=f32
    ).astype(bf16)
    grad_tok = dot_nt(grad_hidden, whole_skip[:d])[:rows].astype(bf16)
    grad_skp = dot_nt(grad_hidden, whole_skip[d:])[:rows].astype(bf16)
    vector_grads = jnp.stack(
        [
            jnp.sum(grad_one * unit_one, 0),
            jnp.sum(grad_two * unit_two, 0),
            jnp.sum(grad_hidden.astype(f32), 0),
            jnp.sum(grad_one, 0),
            jnp.sum(grad_attention.astype(f32), 0),
            jnp.sum(grad_two, 0),
            jnp.sum(dy32, 0),
        ]
    )
    vector_grads = vector_grads.reshape(7, dp, mp, cols).transpose(2, 1, 0, 3)
    vector_grads = vector_grads.reshape(mp, dp, 7 * cols)
    grad_skip = grad_skip.reshape(dp, mp, part, d)
    pieces = []
    for j in range(mp):
        piece = lax.dynamic_slice(grad_skip, (0, my ^ j, 0, 0), (dp, 1, part, d))[:, 0]
        line = lax.dynamic_slice(vector_grads, (my ^ j, 0, 0), (1, dp, 7 * cols))[0]
        line = jnp.concatenate([line, grad_up_bias[j]], 1)
        line = jnp.pad(line[:, None], ((0, 0), (0, 7), (0, d - line.shape[1]))).astype(bf16)
        pieces.append(jnp.concatenate([piece, line], 1).reshape(dp * span, d))
    got = swap(jnp.stack(pieces[1::2]), 1, mp)
    tail = {2 * n: add(pieces[2 * n], got[n]).astype(bf16) for n in range(mp // 2)}
    tail = scatter_blocks(tail, order_a[:-1], mp)
    tail = line_scatter(tail.reshape(dp, span, d))
    skip_grads = tail[:part]
    line = tail[part]
    gain_grads = line[: 2 * cols].reshape(2, cols)
    shift_grads = line[2 * cols : 7 * cols].reshape(5, cols)
    up_bias_grads = line[7 * cols : 7 * cols + hidden_part]
    return (
        output,
        grad_tok,
        grad_skp,
        skip_grads,
        gain_grads,
        shift_grads,
        in_grads,
        out_grads,
        up_grads,
        up_bias_grads,
        down_grads,
    )


def solution(mesh):
    both = P(("dp", "mp"), None)
    last = P(None, ("dp", "mp"))
    in_specs = (
        both, both, P("dp"), both, both, last, last,
        P("dp", None, "mp"), P("mp", "dp"), P("dp", "mp"), P(("mp", "dp")), P("mp", "dp"),
    )
    out_specs = (
        both, both, both, both, last, last,
        P("dp", None, "mp"), P("mp", "dp"), P("dp", "mp"), P(("mp", "dp")), P("mp", "dp"),
    )
    return jax.shard_map(shards, mesh=mesh, in_specs=in_specs, out_specs=out_specs, check_vma=False)
```
